32 devices in a mesh: node: 16 (over z, x, core), tp: 2 (over y).
Axes of the slice: x: 2, y: 2, z: 4, core: 2. Of those that a mesh axis runs over, the one named last changes fastest.
Arguments:
- states: bfloat16 [16, 448, 4096], P('node', None, 'tp'), may hold values from -40 to 40
- weights: bfloat16 [16, 4096, 384], P('node', 'tp'), may hold values from -66 to 66
- norm_gain: float32 [4096], P('tp'), may hold values from 0.1 to 1.9
- cotangent: bfloat16 [16, 448, 128], P('node'), may hold values from -6 to 6
- round_index: int32 [1], replicated, may hold values from 0 to 999
Outputs:
- new_weights: bfloat16 [16, 4096, 384], P('node', 'tp')
The draws below stay inside these ranges and needn't reach their ends.
All inputs are finite; a program needn't handle non-finite values.
Results may differ from the reference program's by a relative error of at most 0.0095.
Values may be sent and summed in bfloat16 or wider, within the bound.
A program may use at most 64 MiB of HBM per device.

```python
import math
import jax
import jax.numpy as jnp
from jax import lax

D = 4096
HD = 128
TOK = 448
NODES = 16
N_NODE = 16


def draw_states(key, part):
    noise_key, jitter_key = jax.random.split(key, 2)
    position = jnp.arange(D, dtype=jnp.float32)
    jitter = jax.random.uniform(jitter_key, (NODES, 1, D), dtype=jnp.float32)
    scales = jnp.exp(jnp.log(10.0) * (position + jitter) / D)
    entries = jax.random.truncated_normal(noise_key, -4.0, 4.0, (NODES, TOK, D), jnp.float32)
    return (entries * scales).astype(jnp.bfloat16)


def draw_weights(key, part):
    base_key = jax.random.fold_in(key, 0)
    entries = jax.random.truncated_normal(base_key, -4.0, 4.0, (NODES, D, 3 * HD), jnp.float32)
    return entries.astype(jnp.bfloat16)


def level_of(stream_key, shape, cuts, smallest, high):
    factor_of, own = 1.0, jax.random.fold_in(stream_key, 6)
    for dim, parts in cuts:
        draws = jnp.exp(jax.random.uniform(jax.random.fold_in(own, dim), (parts,), jnp.float32, smallest / len(cuts), high / len(cuts)))
        factor_of = factor_of * jnp.repeat(draws, shape[dim] // parts).reshape([-1 if axis == dim else 1 for axis in range(len(shape))])
    return factor_of


def bell_draw(stream_key, shape, scale, reach, shards=(), kind=jnp.bfloat16):
    array = jax.random.normal(stream_key, shape, jnp.float32) * scale
    if len(shards) > 0:
        array = level_of(stream_key, shape, shards, -0.22, 0.18) * array
    return jnp.clip(array, min=-reach, max=reach).astype(kind)


def setup_inputs(seed: int = 0) -> dict:
    splits = jax.random.split(jax.random.key(seed), 6)
    return {
        "states": draw_states(jax.random.fold_in(splits[5], 71), 0),
        "weights": draw_weights(jax.random.fold_in(splits[5], 71), 0),
        "norm_gain": jnp.clip(1.0 + 0.18 * jax.random.normal(splits[2], (D,), jnp.float32), 0.1, 1.9),
        "cotangent": bell_draw(splits[3], (NODES, TOK, HD), 1.0, 6.0, ((0, 16),)),
        "round_index": jax.random.randint(splits[4], (1,), 0, 1000).astype(jnp.int32),
    }


rate = 0.5
norm_eps = 1e-05
step_eps = 1e-06

def contract(left, right, left_dim, right_dim):
    return lax.dot_general(left, right, (((left_dim,), (right_dim,)), ((), ())), preferred_element_type=jnp.float32)

def rope_tables(length, width):
    half_width = width // 2
    exponents = jnp.arange(half_width, dtype=jnp.float32) * (2.0 / width)
    frequency = jnp.exp(-jnp.log(jnp.float32(500000.0)) * exponents)
    angles = jnp.arange(length, dtype=jnp.float32)[:, None] * frequency[None, :]
    return (jnp.cos(angles), jnp.sin(angles))

def rotate(entries, cosine_table, sine_table):
    half_width = entries.shape[1] // 2
    leading = entries[:, :half_width]
    trailing = entries[:, half_width:]
    return jnp.concatenate([leading * cosine_table - trailing * sine_table, trailing * cosine_table + leading * sine_table], axis=1)

def unrotate(entries, cosine_table, sine_table):
    half_width = entries.shape[1] // 2
    leading = entries[:, :half_width]
    trailing = entries[:, half_width:]
    return jnp.concatenate([leading * cosine_table + trailing * sine_table, trailing * cosine_table - leading * sine_table], axis=1)

def attend_backward(projected, inv_rms, upstream):
    length = projected.shape[0]
    width = upstream.shape[1]
    cosine_table, sine_table = rope_tables(length, width)
    scaled = projected * inv_rms[:, None]
    queries = rotate(scaled[:, :width], cosine_table, sine_table).astype(jnp.bfloat16)
    keys = rotate(scaled[:, width:2 * width], cosine_table, sine_table).astype(jnp.bfloat16)
    values = scaled[:, 2 * width:].astype(jnp.bfloat16)
    scale_factor = 1.0 / math.sqrt(width)
    scores = contract(queries, keys, 1, 1) * scale_factor
    row_ids = jnp.arange(length, dtype=jnp.int32)
    causal = row_ids[None, :] <= row_ids[:, None]
    scores = jnp.where(causal, scores, -1e+30)
    peak = lax.optimization_barrier(jnp.max(scores, axis=1, keepdims=True))
    lifted = jnp.where(causal, jnp.exp(scores - peak), 0.0)
    probs = lifted / lax.optimization_barrier(jnp.sum(lifted, axis=1, keepdims=True))
    probs_low = probs.astype(jnp.bfloat16)
    attended = jnp.dot(probs_low, values, preferred_element_type=jnp.float32)
    row_dots = lax.optimization_barrier(jnp.sum(attended * upstream.astype(jnp.float32), axis=1))
    dvalues = contract(probs_low, upstream, 0, 0)
    dprobs = contract(upstream, values, 1, 1)
    dscores = (probs * (dprobs - row_dots[:, None]) * scale_factor).astype(jnp.bfloat16)
    dqueries = jnp.dot(dscores, keys, preferred_element_type=jnp.float32)
    dkeys = contract(dscores, queries, 0, 0)
    slope = jnp.concatenate([unrotate(dqueries, cosine_table, sine_table), unrotate(dkeys, cosine_table, sine_table), dvalues], axis=1)
    return (slope * inv_rms[:, None]).astype(jnp.bfloat16)

def take_step(weight_block, gradient, total, count):
    rms_value = jnp.sqrt(total / count + step_eps)
    return (weight_block.astype(jnp.float32) - rate * gradient / rms_value).astype(jnp.bfloat16)

def reference(states, weights, norm_gain, cotangent, round_index):

    def one_node(items):
        node_states, node_weights, upstream = items
        states_f32 = node_states.astype(jnp.float32)
        gained = (states_f32 * norm_gain).astype(jnp.bfloat16)
        projected = jnp.dot(gained, node_weights, preferred_element_type=jnp.float32) / math.sqrt(D)
        squares = lax.optimization_barrier(jnp.sum(states_f32 * states_f32, axis=1))
        inv_rms = lax.rsqrt(squares / D + norm_eps)
        slope = attend_backward(projected, inv_rms, upstream)
        gradient = contract(gained, slope, 0, 0)
        total = jnp.sum(gradient * gradient)
        return take_step(node_weights, gradient, total, D * 3 * HD)
    stepped = lax.map(one_node, (states, weights, cotangent))
    levels = N_NODE.bit_length() - 1
    offset = jnp.left_shift(jnp.int32(1), (round_index[0] % levels).astype(jnp.int32))
    partner = jnp.roll(stepped, offset, axis=0)
    return ((stepped.astype(jnp.float32) + partner.astype(jnp.float32)) * 0.5).astype(jnp.bfloat16)
```

```python
import functools
import math

import jax
import jax.numpy as jnp
import numpy as np
from jax import lax
from jax.experimental import pallas as pl
from jax.experimental.pallas import tpu as pltpu
from jax.sharding import PartitionSpec as P

rate = 0.5
norm_eps = 1e-05
step_eps = 1e-06
MESH = pl.DeviceIdType.MESH
F32 = jnp.float32
BF16 = jnp.bfloat16


def contract(left, right, left_dim, right_dim):
    return lax.dot_general(
        left, right, (((left_dim,), (right_dim,)), ((), ())), preferred_element_type=F32
    )


def rope_tables(length, width):
    half_width = width // 2
    exponents = np.arange(half_width, dtype=np.float64) * (2.0 / width)
    frequency = np.exp(-np.log(500000.0) * exponents)
    angles = np.arange(length, dtype=np.float64)[:, None] * frequency[None, :]
    cosine, sine = np.cos(angles), np.sin(angles)
    return (
        np.concatenate([cosine, cosine], axis=1).astype(np.float32),
        np.concatenate([-sine, sine], axis=1).astype(np.float32),
    )


def split(total, pieces):
    return [(i * (total // pieces), total // pieces) for i in range(pieces)]


def kernel(
    n_nodes, n_tp, offset,
    states_hbm, weights_hbm, gain_ref, cot_ref, cos_ref, sin_ref,
    out_hbm,
    states_v, weights_v, gained_v, gained_t, part_v, part_send, part_recv,
    sq_send, sq_recv, tot_send, tot_recv, slope_v, grad_v, step_v, recv_v, out_v,
    load_sem, part_ssem, part_rsem, sq_sem, tot_sem, step_ssem, step_rsem, out_sem,
):
    tokens, local = states_v.shape
    columns = weights_v.shape[1]
    width = columns // 3
    features = local * n_tp
    row_blocks = split(tokens, part_ssem.shape[0])
    chunks = split(local, step_ssem.shape[0])
    me, my_tp = lax.axis_index("node"), lax.axis_index("tp")
    target = lax.rem(me + offset, n_nodes)
    source = lax.rem(me - offset + n_nodes, n_nodes)
    other = lax.rem(my_tp + 1, n_tp)

    barrier = pltpu.get_barrier_semaphore()
    pl.semaphore_signal(barrier, inc=1, device_id={"tp": other}, device_id_type=MESH)
    pl.semaphore_signal(barrier, inc=1, device_id={"node": target}, device_id_type=MESH)
    greeted = 2
    if 2 * offset != n_nodes:
        pl.semaphore_signal(barrier, inc=1, device_id={"node": source}, device_id_type=MESH)
        greeted = 3

    loads = [pltpu.make_async_copy(weights_hbm, weights_v, load_sem.at[len(row_blocks)])]
    for i, (start, size) in enumerate(row_blocks):
        rows = pl.ds(start, size)
        loads.append(pltpu.make_async_copy(states_hbm.at[rows], states_v.at[rows], load_sem.at[i]))
    for load in loads:
        load.start()

    def part_copy(i):
        rows = pl.ds(*row_blocks[i])
        return pltpu.make_async_remote_copy(
            part_send.at[rows], part_recv.at[rows], part_ssem.at[i], part_rsem.at[i],
            device_id={"tp": other}, device_id_type=MESH,
        )

    def step_copy(i):
        rows = pl.ds(*chunks[i])
        return pltpu.make_async_remote_copy(
            step_v.at[rows], recv_v.at[rows], step_ssem.at[i], step_rsem.at[i],
            device_id={"node": target}, device_id_type=MESH,
        )

    sq_copy = pltpu.make_async_remote_copy(
        sq_send, sq_recv, sq_sem.at[0], sq_sem.at[1], device_id={"tp": other}, device_id_type=MESH
    )
    tot_copy = pltpu.make_async_remote_copy(
        tot_send, tot_recv, tot_sem.at[0], tot_sem.at[1], device_id={"tp": other}, device_id_type=MESH
    )

    gain = gain_ref[...]
    squares = []
    for i, (start, size) in enumerate(row_blocks):
        rows = pl.ds(start, size)
        loads[i + 1].wait()
        wide = states_v[rows, :].astype(F32)
        gained = (wide * gain).astype(BF16)
        gained_v[rows, :] = gained
        squares.append(jnp.sum(wide * wide, axis=1, keepdims=True))
        if i == 0:
            loads[0].wait()
        partial = jnp.dot(gained, weights_v[...], preferred_element_type=F32)
        part_v[rows, :] = partial
        part_send[rows, :] = partial.astype(BF16)
        if i == 1:
            pl.semaphore_wait(barrier, greeted)
        if i >= 1:
            part_copy(i - 1).start()
    squares = jnp.concatenate(squares, axis=0)
    row_ids = lax.broadcasted_iota(jnp.int32, (tokens, tokens), 0)
    key_ids = lax.broadcasted_iota(jnp.int32, (tokens, tokens), 1)
    diagonal = row_ids == key_ids
    as_row = jnp.sum(jnp.where(diagonal, squares, 0.0), axis=0, keepdims=True)
    sq_send[...] = jnp.broadcast_to(as_row, sq_send.shape)
    part_copy(len(row_blocks) - 1).start()

    for start, size in chunks:
        gained_t[pl.ds(start, size), :] = gained_v[:, pl.ds(start, size)].T
    sq_copy.start()

    for i in range(len(row_blocks)):
        part_copy(i).wait()
    sq_copy.wait()
    their_squares = jnp.sum(
        jnp.where(diagonal, sq_recv[0:1, :], 0.0), axis=1, keepdims=True
    )
    inv_rms = lax.rsqrt((squares + their_squares) / features + norm_eps)
    row_scale = inv_rms * (1.0 / math.sqrt(features))
    cosine, sine = cos_ref[...], sin_ref[...]
    half = width // 2

    def block(index):
        lanes = pl.ds(index * width, width)
        return (part_v[:, lanes] + part_recv[:, lanes].astype(F32)) * row_scale

    def rotate(entries):
        return entries * cosine + pltpu.roll(entries, half, 1) * sine

    def unrotate(entries):
        return entries * cosine - pltpu.roll(entries, half, 1) * sine

    queries = rotate(block(0)).astype(BF16)
    keys = rotate(block(1)).astype(BF16)
    values = block(2).astype(BF16)
    upstream = cot_ref[...]
    scale_factor = 1.0 / math.sqrt(width)
    causal = key_ids <= row_ids
    scores = jnp.where(causal, contract(queries, keys, 1, 1) * scale_factor, -1e30)
    peak = jnp.max(scores, axis=1, keepdims=True)
    lifted = jnp.where(causal, jnp.exp(scores - peak), 0.0)
    probs = lifted * (1.0 / jnp.sum(lifted, axis=1, keepdims=True))
    probs_low = probs.astype(BF16)
    dprobs = contract(upstream, values, 1, 1)
    row_dots = jnp.sum(probs_low.astype(F32) * dprobs, axis=1, keepdims=True)
    dscores = (probs * (dprobs - row_dots) * scale_factor).astype(BF16)
    dvalues = contract(probs_low, upstream, 0, 0)
    dqueries = jnp.dot(dscores, keys, preferred_element_type=F32)
    dkeys = contract(dscores, queries, 0, 0)
    slope_v[:, pl.ds(0, width)] = (unrotate(dqueries) * inv_rms).astype(BF16)
    slope_v[:, pl.ds(width, width)] = (unrotate(dkeys) * inv_rms).astype(BF16)
    slope_v[:, pl.ds(2 * width, width)] = (dvalues * inv_rms).astype(BF16)

    total = jnp.zeros((8, columns), F32)
    for start, size in chunks:
        rows = pl.ds(start, size)
        gradient = jnp.dot(gained_t[rows, :], slope_v[...], preferred_element_type=F32)
        grad_v[rows, :] = gradient
        total += jnp.sum((gradient * gradient).reshape(size // 8, 8, columns), axis=0)
    total = jnp.sum(jnp.sum(total, axis=0, keepdims=True), axis=1, keepdims=True)
    tot_send[...] = jnp.broadcast_to(total, tot_send.shape)
    tot_copy.start()
    tot_copy.wait()
    mean_square = (total + tot_recv[0:1, 0:1]) / (features * columns)
    factor = rate * lax.rsqrt(mean_square + step_eps)

    for i, (start, size) in enumerate(chunks):
        rows = pl.ds(start, size)
        step_v[rows, :] = (weights_v[rows, :].astype(F32) - grad_v[rows, :] * factor).astype(BF16)
        if i >= 1:
            step_copy(i - 1).start()
    step_copy(len(chunks) - 1).start()

    outs = []
    for i, (start, size) in enumerate(chunks):
        rows = pl.ds(start, size)
        step_copy(i).wait_recv()
        both = step_v[rows, :].astype(F32) + recv_v[rows, :].astype(F32)
        out_v[rows, :] = (both * 0.5).astype(BF16)
        outs.append(pltpu.make_async_copy(out_v.at[rows], out_hbm.at[rows], out_sem.at[i]))
        outs[-1].start()
    for i in range(len(chunks)):
        step_copy(i).wait_send()
        outs[i].wait()


def one_round(n_nodes, n_tp, level, states, weights, gain, upstream, cosine, sine):
    tokens, local = states.shape
    columns = weights.shape[1]
    pieces, parts = 16, 4
    vmem = pl.BlockSpec(memory_space=pltpu.VMEM)
    anywhere = pl.BlockSpec(memory_space=pl.ANY)
    dma = pltpu.SemaphoreType.DMA
    flops = 4 * tokens * local * columns + 12 * tokens * tokens * columns // 3
    return pl.pallas_call(
        functools.partial(kernel, n_nodes, n_tp, 1 << level),
        out_shape=jax.ShapeDtypeStruct(weights.shape, BF16),
        in_specs=[anywhere, anywhere, vmem, vmem, vmem, vmem],
        out_specs=anywhere,
        scratch_shapes=[
            pltpu.VMEM((tokens, local), BF16),
            pltpu.VMEM((local, columns), BF16),
            pltpu.VMEM((tokens, local), BF16),
            pltpu.VMEM((local, tokens), BF16),
            pltpu.VMEM((tokens, columns), F32),
            pltpu.VMEM((tokens, columns), BF16),
            pltpu.VMEM((tokens, columns), BF16),
            pltpu.VMEM((8, tokens), F32),
            pltpu.VMEM((8, tokens), F32),
            pltpu.VMEM((8, 128), F32),
            pltpu.VMEM((8, 128), F32),
            pltpu.VMEM((tokens, columns), BF16),
            pltpu.VMEM((local, columns), F32),
            pltpu.VMEM((local, columns), BF16),
            pltpu.VMEM((local, columns), BF16),
            pltpu.VMEM((local, columns), BF16),
            dma((parts + 1,)),
            dma((parts,)),
            dma((parts,)),
            dma((2,)),
            dma((2,)),
            dma((pieces,)),
            dma((pieces,)),
            dma((pieces,)),
        ],
        compiler_params=pltpu.CompilerParams(
            collective_id=level, has_side_effects=True, vmem_limit_bytes=60 * 2**20
        ),
        cost_estimate=pl.CostEstimate(
            flops=flops, bytes_accessed=6 * local * columns + 2 * tokens * local, transcendentals=0
        ),
        name="gossip",
    )(states, weights, gain, upstream, cosine, sine)


def solution(mesh):
    n_nodes, n_tp = mesh.shape["node"], mesh.shape["tp"]
    levels = n_nodes.bit_length() - 1

    def per_device(states, weights, norm_gain, cotangent, round_index):
        cosine, sine = rope_tables(cotangent.shape[1], cotangent.shape[2])
        exponent = round_index[0] % levels
        branches = [functools.partial(one_round, n_nodes, n_tp, level) for level in range(levels)]
        out = lax.switch(
            exponent, branches,
            states[0], weights[0], norm_gain[None, :], cotangent[0], cosine, sine,
        )
        return out[None]

    return jax.shard_map(
        per_device,
        mesh=mesh,
        in_specs=(
            P("node", None, "tp"),
            P("node", "tp", None),
            P("tp"),
            P("node", None, None),
            P(),
        ),
        out_specs=P("node", "tp", None),
        check_vma=False,
    )
```

```python
import functools
import math

import jax
import jax.numpy as jnp
import numpy as np
from jax import lax
from jax.experimental import pallas as pl
from jax.experimental.pallas import tpu as pltpu
from jax.sharding import PartitionSpec as P

rate = 0.5
norm_eps = 1e-05
step_eps = 1e-06
MESH = pl.DeviceIdType.MESH
F32 = jnp.float32
BF16 = jnp.bfloat16


def contract(left, right, left_dim, right_dim):
    return lax.dot_general(
        left, right, (((left_dim,), (right_dim,)), ((), ())), preferred_element_type=F32
    )


def rope_tables(length, width):
    half_width = width // 2
    exponents = np.arange(half_width, dtype=np.float64) * (2.0 / width)
    frequency = np.exp(-np.log(500000.0) * exponents)
    angles = np.arange(length, dtype=np.float64)[:, None] * frequency[None, :]
    cosine, sine = np.cos(angles), np.sin(angles)
    return (
        np.concatenate([cosine, cosine], axis=1).astype(np.float32),
        np.concatenate([-sine, sine], axis=1).astype(np.float32),
    )


def token_blocks(tokens):
    return [(start, min(128, tokens - start)) for start in range(0, tokens, 128)]


def split(total, pieces):
    return [(i * (total // pieces), total // pieces) for i in range(pieces)]


def kernel(
    n_nodes, n_tp, offset,
    states_hbm, weights_hbm, gain_hbm, cot_hbm, cos_hbm, sin_hbm,
    out_ref,
    states_v, weights_v, gain_ref, cot_ref, cos_ref, sin_ref,
    gained_v, gained_t, part_v, part_send, part_recv,
    sq_send, sq_recv, tot_send, tot_recv, keys_v, values_v, dkeys_v, dvalues_v,
    slope_v, grad_v, step_v, recv_v,
    load_sem, part_ssem, part_rsem, sq_ssem, sq_rsem, tot_sem, step_ssem, step_rsem,
):
    tokens, local = states_v.shape
    columns = weights_v.shape[1]
    width = columns // 3
    features = local * n_tp
    row_blocks = token_blocks(tokens)
    chunks = split(local, step_ssem.shape[0])
    me, my_tp = lax.axis_index("node"), lax.axis_index("tp")
    target = lax.rem(me + offset, n_nodes)
    source = lax.rem(me - offset + n_nodes, n_nodes)
    other = lax.rem(my_tp + 1, n_tp)

    barrier = pltpu.get_barrier_semaphore()
    pl.semaphore_signal(barrier, inc=1, device_id={"tp": other}, device_id_type=MESH)
    pl.semaphore_signal(barrier, inc=1, device_id={"node": target}, device_id_type=MESH)
    greeted = 2
    if 2 * offset != n_nodes:
        pl.semaphore_signal(barrier, inc=1, device_id={"node": source}, device_id_type=MESH)
        greeted = 3

    loads = [pltpu.make_async_copy(weights_hbm, weights_v, load_sem.at[len(row_blocks)])]
    for i, (start, size) in enumerate(row_blocks):
        rows = pl.ds(start, size)
        loads.append(pltpu.make_async_copy(states_hbm.at[rows], states_v.at[rows], load_sem.at[i]))
    small = len(row_blocks) + 1
    for i, (there, here) in enumerate(
        [(gain_hbm, gain_ref), (cot_hbm, cot_ref), (cos_hbm, cos_ref), (sin_hbm, sin_ref)]
    ):
        loads.append(pltpu.make_async_copy(there, here, load_sem.at[small + i]))
    loads[small].start()
    for i in [1, 0] + list(range(2, len(loads))):
        if i != small:
            loads[i].start()

    def part_copy(i):
        rows = pl.ds(*row_blocks[i])
        return pltpu.make_async_remote_copy(
            part_send.at[rows], part_recv.at[rows], part_ssem.at[i], part_rsem.at[i],
            device_id={"tp": other}, device_id_type=MESH,
        )

    def step_copy(i):
        rows = pl.ds(*chunks[i])
        return pltpu.make_async_remote_copy(
            step_v.at[rows], recv_v.at[rows], step_ssem.at[i], step_rsem.at[i],
            device_id={"node": target}, device_id_type=MESH,
        )

    def sq_copy(i):
        return pltpu.make_async_remote_copy(
            sq_send.at[i], sq_recv.at[i], sq_ssem.at[i], sq_rsem.at[i],
            device_id={"tp": other}, device_id_type=MESH,
        )

    tot_copy = pltpu.make_async_remote_copy(
        tot_send, tot_recv, tot_sem.at[0], tot_sem.at[1], device_id={"tp": other}, device_id_type=MESH
    )

    def diagonal(size):
        shape = (size, 128)
        return lax.broadcasted_iota(jnp.int32, shape, 0) == lax.broadcasted_iota(jnp.int32, shape, 1)

    loads[small].wait()
    gain = gain_ref[...]
    squares = []
    for i, (start, size) in enumerate(row_blocks):
        rows = pl.ds(start, size)
        loads[i + 1].wait()
        wide = states_v[rows, :].astype(F32)
        gained = (wide * gain).astype(BF16)
        gained_v[rows, :] = gained
        squares.append(jnp.sum(wide * wide, axis=1, keepdims=True))
        as_row = jnp.sum(jnp.where(diagonal(size), squares[i], 0.0), axis=0, keepdims=True)
        sq_send[i] = jnp.broadcast_to(as_row, (8, 128))
        if i == 0:
            loads[0].wait()
        partial = jnp.dot(gained, weights_v[...], preferred_element_type=F32)
        part_v[rows, :] = partial
        part_send[rows, :] = partial.astype(BF16)
        if i == 1:
            pl.semaphore_wait(barrier, greeted)
        if i >= 1:
            sq_copy(i - 1).start()
            part_copy(i - 1).start()
    last = len(row_blocks) - 1
    sq_copy(last).start()
    part_copy(last).start()

    for start, size in chunks:
        gained_t[pl.ds(start, size), :] = gained_v[:, pl.ds(start, size)].T
    for i in range(small + 1, small + 4):
        loads[i].wait()

    half = width // 2
    scale_factor = 1.0 / math.sqrt(width)
    inverses = []
    for i, (start, size) in enumerate(row_blocks):
        rows, seen = pl.ds(start, size), start + size
        sq_copy(i).wait()
        theirs = jnp.sum(jnp.where(diagonal(size), sq_recv[i, 0:1, :], 0.0), axis=1, keepdims=True)
        inv_rms = lax.rsqrt((squares[i] + theirs) / features + norm_eps)
        inverses.append(inv_rms)
        row_scale = inv_rms * (1.0 / math.sqrt(features))
        cosine, sine = cos_ref[rows, :], sin_ref[rows, :]
        part_copy(i).wait()

        def block(index):
            lanes = pl.ds(index * width, width)
            return (part_v[rows, lanes] + part_recv[rows, lanes].astype(F32)) * row_scale

        def rotate(entries):
            return entries * cosine + pltpu.roll(entries, half, 1) * sine

        queries = rotate(block(0)).astype(BF16)
        keys_v[rows, :] = rotate(block(1)).astype(BF16)
        values_v[rows, :] = block(2).astype(BF16)
        keys, values = keys_v[0:seen, :], values_v[0:seen, :]
        upstream = cot_ref[rows, :]
        row_ids = start + lax.broadcasted_iota(jnp.int32, (size, seen), 0)
        causal = lax.broadcasted_iota(jnp.int32, (size, seen), 1) <= row_ids
        scores = jnp.where(causal, contract(queries, keys, 1, 1) * scale_factor, -1e30)
        dprobs = contract(upstream, values, 1, 1)
        peak = jnp.max(scores, axis=1, keepdims=True)
        lifted = jnp.where(causal, jnp.exp(scores - peak), 0.0)
        probs = lifted * (1.0 / jnp.sum(lifted, axis=1, keepdims=True))
        probs_low = probs.astype(BF16)
        row_dots = jnp.sum(probs_low.astype(F32) * dprobs, axis=1, keepdims=True)
        dscores = (probs * (dprobs - row_dots) * scale_factor).astype(BF16)
        dvalues = contract(probs_low, upstream, 0, 0)
        dkeys = contract(dscores, queries, 0, 0)
        if i > 0:
            dvalues_v[0:start, :] += dvalues[:start]
            dkeys_v[0:start, :] += dkeys[:start]
        dvalues_v[rows, :] = dvalues[start:]
        dkeys_v[rows, :] = dkeys[start:]
        dqueries = jnp.dot(dscores, keys, preferred_element_type=F32)
        dqueries = dqueries * cosine - pltpu.roll(dqueries, half, 1) * sine
        slope_v[rows, pl.ds(0, width)] = (dqueries * inv_rms).astype(BF16)
    for i, (start, size) in enumerate(row_blocks):
        rows = pl.ds(start, size)
        dkeys = dkeys_v[rows, :]
        dkeys = dkeys * cos_ref[rows, :] - pltpu.roll(dkeys, half, 1) * sin_ref[rows, :]
        slope_v[rows, pl.ds(width, width)] = (dkeys * inverses[i]).astype(BF16)
        slope_v[rows, pl.ds(2 * width, width)] = (dvalues_v[rows, :] * inverses[i]).astype(BF16)

    total = jnp.zeros((8, columns), F32)
    for start, size in chunks:
        rows = pl.ds(start, size)
        gradient = jnp.dot(gained_t[rows, :], slope_v[...], preferred_element_type=F32)
        grad_v[rows, :] = gradient
        total += jnp.sum((gradient * gradient).reshape(size // 8, 8, columns), axis=0)
    total = jnp.sum(jnp.sum(total, axis=0, keepdims=True), axis=1, keepdims=True)
    tot_send[...] = jnp.broadcast_to(total, tot_send.shape)
    tot_copy.start()
    tot_copy.wait()
    mean_square = (total + tot_recv[0:1, 0:1]) / (features * columns)
    factor = rate * lax.rsqrt(mean_square + step_eps)

    for i, (start, size) in enumerate(chunks):
        rows = pl.ds(start, size)
        step_v[rows, :] = (weights_v[rows, :].astype(F32) - grad_v[rows, :] * factor).astype(BF16)
        if i >= 1:
            step_copy(i - 1).start()
    step_copy(len(chunks) - 1).start()

    for i, (start, size) in enumerate(chunks):
        rows = pl.ds(start, size)
        step_copy(i).wait_recv()
        both = step_v[rows, :].astype(F32) + recv_v[rows, :].astype(F32)
        out_ref[rows, :] = (both * 0.5).astype(BF16)
    for i in range(len(chunks)):
        step_copy(i).wait_send()


def one_round(n_nodes, n_tp, level, states, weights, gain, upstream, cosine, sine):
    tokens, local = states.shape
    columns = weights.shape[1]
    width = columns // 3
    pieces, parts = 16, len(token_blocks(tokens))
    vmem = pl.BlockSpec(memory_space=pltpu.VMEM)
    anywhere = pl.BlockSpec(memory_space=pl.ANY)
    dma = pltpu.SemaphoreType.DMA
    flops = 4 * tokens * local * columns + 12 * tokens * tokens * columns // 3
    return pl.pallas_call(
        functools.partial(kernel, n_nodes, n_tp, 1 << level),
        out_shape=jax.ShapeDtypeStruct(weights.shape, BF16),
        in_specs=[anywhere] * 6,
        out_specs=vmem,
        scratch_shapes=[
            pltpu.VMEM((tokens, local), BF16),
            pltpu.VMEM((local, columns), BF16),
            pltpu.VMEM(gain.shape, F32),
            pltpu.VMEM((tokens, width), BF16),
            pltpu.VMEM((tokens, width), F32),
            pltpu.VMEM((tokens, width), F32),
            pltpu.VMEM((tokens, local), BF16),
            pltpu.VMEM((local, tokens), BF16),
            pltpu.VMEM((tokens, columns), F32),
            pltpu.VMEM((tokens, columns), BF16),
            pltpu.VMEM((tokens, columns), BF16),
            pltpu.VMEM((parts, 8, 128), F32),
            pltpu.VMEM((parts, 8, 128), F32),
            pltpu.VMEM((8, 128), F32),
            pltpu.VMEM((8, 128), F32),
            pltpu.VMEM((tokens, width), BF16),
            pltpu.VMEM((tokens, width), BF16),
            pltpu.VMEM((tokens, width), F32),
            pltpu.VMEM((tokens, width), F32),
            pltpu.VMEM((tokens, columns), BF16),
            pltpu.VMEM((local, columns), F32),
            pltpu.VMEM((local, columns), BF16),
            pltpu.VMEM((local, columns), BF16),
            dma((parts + 5,)),
            dma((parts,)),
            dma((parts,)),
            dma((parts,)),
            dma((parts,)),
            dma((2,)),
            dma((pieces,)),
            dma((pieces,)),
        ],
        compiler_params=pltpu.CompilerParams(
            collective_id=level, has_side_effects=True, vmem_limit_bytes=60 * 2**20
        ),
        cost_estimate=pl.CostEstimate(
            flops=flops, bytes_accessed=6 * local * columns + 2 * tokens * local, transcendentals=0
        ),
        name="gossip",
    )(states, weights, gain, upstream, cosine, sine)


def solution(mesh):
    n_nodes, n_tp = mesh.shape["node"], mesh.shape["tp"]
    levels = n_nodes.bit_length() - 1

    def per_device(states, weights, norm_gain, cotangent, round_index):
        cosine, sine = rope_tables(cotangent.shape[1], cotangent.shape[2])
        exponent = round_index[0] % levels
        branches = [functools.partial(one_round, n_nodes, n_tp, level) for level in range(levels)]
        out = lax.switch(
            exponent, branches,
            states[0], weights[0], norm_gain[None, :], cotangent[0], cosine, sine,
        )
        return out[None]

    return jax.shard_map(
        per_device,
        mesh=mesh,
        in_specs=(
            P("node", None, "tp"),
            P("node", "tp", None),
            P("tp"),
            P("node", None, None),
            P(),
        ),
        out_specs=P("node", "tp", None),
        check_vma=False,
    )
```

```python
import functools
import math

import jax
import jax.numpy as jnp
import numpy as np
from jax import lax
from jax.experimental import pallas as pl
from jax.experimental.pallas import tpu as pltpu
from jax.sharding import PartitionSpec as P

rate = 0.5
norm_eps = 1e-05
step_eps = 1e-06
MESH = pl.DeviceIdType.MESH
F32 = jnp.float32
BF16 = jnp.bfloat16


def contract(left, right, left_dim, right_dim):
    return lax.dot_general(
        left, right, (((left_dim,), (right_dim,)), ((), ())), preferred_element_type=F32
    )


def rope_tables(length, width):
    half_width = width // 2
    exponents = np.arange(half_width, dtype=np.float64) * (2.0 / width)
    frequency = np.exp(-np.log(500000.0) * exponents)
    angles = np.arange(length, dtype=np.float64)[:, None] * frequency[None, :]
    cosine, sine = np.cos(angles), np.sin(angles)
    return (
        np.concatenate([cosine, cosine], axis=1).astype(np.float32),
        np.concatenate([-sine, sine], axis=1).astype(np.float32),
    )


def token_blocks(tokens):
    return [(start, min(128, tokens - start)) for start in range(0, tokens, 128)]


def split(total, pieces):
    return [(i * (total // pieces), total // pieces) for i in range(pieces)]


def kernel(
    n_nodes, n_tp, offset, early,
    states_hbm, weights_hbm, gain_hbm, cot_hbm, cos_hbm, sin_hbm,
    out_ref,
    states_v, weights_v, gain_ref, cot_ref, cos_ref, sin_ref,
    gained_v, gained_t, part_v, part_send, part_recv,
    sq_send, sq_recv, tot_send, tot_recv, keys_v, values_v, dkeys_v, dvalues_v,
    slope_v, grad_v, step_v, recv_v,
    early_states, early_weights, early_t, slope_in, fact_send, fact_recv,
    load_sem, part_ssem, part_rsem, sq_ssem, sq_rsem, tot_sem, step_ssem, step_rsem,
    early_ssem, early_rsem, slope_ssem, slope_rsem, fact_sem,
):
    tokens, local = states_v.shape
    columns = weights_v.shape[1]
    width = columns // 3
    features = local * n_tp
    row_blocks = token_blocks(tokens)
    chunks = split(local, step_ssem.shape[0])
    piece = chunks[0][1]
    late = [chunk for chunk in chunks if chunk[0] >= early]
    half_tokens = tokens // n_tp
    me, my_tp = lax.axis_index("node"), lax.axis_index("tp")
    target = lax.rem(me + offset, n_nodes)
    source = lax.rem(me - offset + n_nodes, n_nodes)
    other = lax.rem(my_tp + 1, n_tp)

    barrier = pltpu.get_barrier_semaphore()
    pl.semaphore_signal(barrier, inc=1, device_id={"tp": other}, device_id_type=MESH)
    pl.semaphore_signal(barrier, inc=1, device_id={"node": target}, device_id_type=MESH)
    greeted = 2
    if 2 * offset != n_nodes:
        pl.semaphore_signal(barrier, inc=1, device_id={"node": source}, device_id_type=MESH)
        greeted = 3

    loads = [pltpu.make_async_copy(weights_hbm, weights_v, load_sem.at[len(row_blocks)])]
    for i, (start, size) in enumerate(row_blocks):
        rows = pl.ds(start, size)
        loads.append(pltpu.make_async_copy(states_hbm.at[rows], states_v.at[rows], load_sem.at[i]))
    small = len(row_blocks) + 1
    for i, (there, here) in enumerate(
        [(gain_hbm, gain_ref), (cot_hbm, cot_ref), (cos_hbm, cos_ref), (sin_hbm, sin_ref)]
    ):
        loads.append(pltpu.make_async_copy(there, here, load_sem.at[small + i]))
    loads[small].start()
    for i in [1, 0] + list(range(2, len(loads))):
        if i != small:
            loads[i].start()

    def part_copy(i):
        rows = pl.ds(*row_blocks[i])
        return pltpu.make_async_remote_copy(
            part_send.at[rows], part_recv.at[rows], part_ssem.at[i], part_rsem.at[i],
            device_id={"tp": other}, device_id_type=MESH,
        )

    def step_copy(i):
        rows = pl.ds(*late[i])
        return pltpu.make_async_remote_copy(
            step_v.at[rows], recv_v.at[rows], step_ssem.at[i], step_rsem.at[i],
            device_id={"node": target}, device_id_type=MESH,
        )

    def sq_copy(i):
        return pltpu.make_async_remote_copy(
            sq_send.at[i], sq_recv.at[i], sq_ssem.at[i], sq_rsem.at[i],
            device_id={"tp": other}, device_id_type=MESH,
        )

    def to_target(there, here, ssem, rsem):
        return pltpu.make_async_remote_copy(
            there, here, ssem, rsem, device_id={"node": target}, device_id_type=MESH
        )

    early_w = to_target(
        weights_v.at[pl.ds(0, early)], early_weights, early_ssem.at[0], early_rsem.at[0]
    )
    early_s = to_target(
        states_v.at[:, pl.ds(0, early)], early_states, early_ssem.at[1], early_rsem.at[1]
    )
    mine = pl.ds(pl.multiple_of(my_tp * half_tokens, 16), half_tokens)
    slope_copy = to_target(
        slope_v.at[mine], slope_in.at[mine], slope_ssem.at[0], slope_rsem.at[0]
    )
    slope_pass = pltpu.make_async_remote_copy(
        slope_in.at[mine], slope_in.at[mine], slope_ssem.at[1], slope_rsem.at[1],
        device_id={"tp": other}, device_id_type=MESH,
    )
    fact_copy = to_target(fact_send, fact_recv, fact_sem.at[0], fact_sem.at[1])
    tot_copy = pltpu.make_async_remote_copy(
        tot_send, tot_recv, tot_sem.at[0], tot_sem.at[1], device_id={"tp": other}, device_id_type=MESH
    )

    def diagonal(size):
        shape = (size, 128)
        return lax.broadcasted_iota(jnp.int32, shape, 0) == lax.broadcasted_iota(jnp.int32, shape, 1)

    loads[small].wait()
    gain = gain_ref[...]
    squares = []
    for i, (start, size) in enumerate(row_blocks):
        rows = pl.ds(start, size)
        loads[i + 1].wait()
        wide = states_v[rows, :].astype(F32)
        gained = (wide * gain).astype(BF16)
        gained_v[rows, :] = gained
        squares.append(jnp.sum(wide * wide, axis=1, keepdims=True))
        as_row = jnp.sum(jnp.where(diagonal(size), squares[i], 0.0), axis=0, keepdims=True)
        sq_send[i] = jnp.broadcast_to(as_row, (8, 128))
        if i == 0:
            loads[0].wait()
        partial = jnp.dot(gained, weights_v[...], preferred_element_type=F32)
        part_v[rows, :] = partial
        part_send[rows, :] = partial.astype(BF16)
        if i == 1:
            pl.semaphore_wait(barrier, greeted)
            early_w.start()
        if i >= 1:
            sq_copy(i - 1).start()
            part_copy(i - 1).start()
    early_s.start()
    last = len(row_blocks) - 1
    sq_copy(last).start()
    part_copy(last).start()

    @pl.loop(0, local // piece)
    def _(i):
        span = pl.ds(pl.multiple_of(i * piece, piece), piece)
        gained_t[span, :] = gained_v[:, span].T

    for i in range(small + 1, small + 4):
        loads[i].wait()

    half = width // 2
    scale_factor = 1.0 / math.sqrt(width)
    inverses = []
    for i, (start, size) in enumerate(row_blocks):
        rows, seen = pl.ds(start, size), start + size
        sq_copy(i).wait()
        theirs = jnp.sum(jnp.where(diagonal(size), sq_recv[i, 0:1, :], 0.0), axis=1, keepdims=True)
        inv_rms = lax.rsqrt((squares[i] + theirs) / features + norm_eps)
        inverses.append(inv_rms)
        row_scale = inv_rms * (1.0 / math.sqrt(features))
        cosine, sine = cos_ref[rows, :], sin_ref[rows, :]
        part_copy(i).wait()

        def block(index):
            lanes = pl.ds(index * width, width)
            return (part_v[rows, lanes] + part_recv[rows, lanes].astype(F32)) * row_scale

        def rotate(entries):
            return entries * cosine + pltpu.roll(entries, half, 1) * sine

        queries = rotate(block(0)).astype(BF16)
        keys_v[rows, :] = rotate(block(1)).astype(BF16)
        values_v[rows, :] = block(2).astype(BF16)
        keys, values = keys_v[0:seen, :], values_v[0:seen, :]
        upstream = cot_ref[rows, :]
        row_ids = start + lax.broadcasted_iota(jnp.int32, (size, seen), 0)
        causal = lax.broadcasted_iota(jnp.int32, (size, seen), 1) <= row_ids
        scores = jnp.where(causal, contract(queries, keys, 1, 1) * scale_factor, -1e30)
        dprobs = contract(upstream, values, 1, 1)
        peak = jnp.max(scores, axis=1, keepdims=True)
        lifted = jnp.where(causal, jnp.exp(scores - peak), 0.0)
        probs = lifted * (1.0 / jnp.sum(lifted, axis=1, keepdims=True))
        probs_low = probs.astype(BF16)
        row_dots = jnp.sum(probs_low.astype(F32) * dprobs, axis=1, keepdims=True)
        dscores = (probs * (dprobs - row_dots) * scale_factor).astype(BF16)
        dvalues = contract(probs_low, upstream, 0, 0)
        dkeys = contract(dscores, queries, 0, 0)
        if i > 0:
            dvalues_v[0:start, :] += dvalues[:start]
            dkeys_v[0:start, :] += dkeys[:start]
        dvalues_v[rows, :] = dvalues[start:]
        dkeys_v[rows, :] = dkeys[start:]
        dqueries = jnp.dot(dscores, keys, preferred_element_type=F32)
        dqueries = dqueries * cosine - pltpu.roll(dqueries, half, 1) * sine
        slope_v[rows, pl.ds(0, width)] = (dqueries * inv_rms).astype(BF16)
    for i, (start, size) in enumerate(row_blocks):
        rows = pl.ds(start, size)
        dkeys = dkeys_v[rows, :]
        dkeys = dkeys * cos_ref[rows, :] - pltpu.roll(dkeys, half, 1) * sin_ref[rows, :]
        slope_v[rows, pl.ds(width, width)] = (dkeys * inverses[i]).astype(BF16)
        slope_v[rows, pl.ds(2 * width, width)] = (dvalues_v[rows, :] * inverses[i]).astype(BF16)

    total = jnp.zeros((8, columns), F32)
    for start, size in chunks:
        if start == piece:
            slope_copy.start()
        rows = pl.ds(start, size)
        gradient = jnp.dot(gained_t[rows, :], slope_v[...], preferred_element_type=F32)
        grad_v[rows, :] = gradient
        total += jnp.sum((gradient * gradient).reshape(size // 8, 8, columns), axis=0)
    total = jnp.sum(jnp.sum(total, axis=0, keepdims=True), axis=1, keepdims=True)
    tot_send[...] = jnp.broadcast_to(total, tot_send.shape)
    tot_copy.start()
    tot_copy.wait()
    mean_square = (total + tot_recv[0:1, 0:1]) / (features * columns)
    factor = rate * lax.rsqrt(mean_square + step_eps)

    fact_send[...] = jnp.broadcast_to(factor, fact_send.shape)

    def step(rows):
        step_v[rows, :] = (weights_v[rows, :].astype(F32) - grad_v[rows, :] * factor).astype(BF16)

    for i, (start, size) in enumerate(late):
        step(pl.ds(start, size))
        if i == 1:
            fact_copy.start()
        if i >= 1:
            step_copy(i - 1).start()
    step_copy(len(late) - 1).start()

    slope_copy.wait_recv()
    slope_pass.start()
    early_w.wait_recv()
    early_s.wait_recv()

    @pl.loop(0, early // piece)
    def _(i):
        span = pl.ds(pl.multiple_of(i * piece, piece), piece)
        step(span)
        gained = (early_states[:, span].astype(F32) * gain_ref[:, span]).astype(BF16)
        early_t[span, :] = gained.T

    slope_pass.wait_recv()
    fact_copy.wait_recv()
    their_factor = fact_recv[0:1, 0:1]

    @pl.loop(0, early // piece)
    def _(i):
        span = pl.ds(pl.multiple_of(i * piece, piece), piece)
        gradient = jnp.dot(early_t[span, :], slope_in[...], preferred_element_type=F32)
        theirs = (early_weights[span, :].astype(F32) - gradient * their_factor).astype(BF16)
        both = step_v[span, :].astype(F32) + theirs.astype(F32)
        out_ref[span, :] = (both * 0.5).astype(BF16)

    for i, (start, size) in enumerate(late):
        rows = pl.ds(start, size)
        step_copy(i).wait_recv()
        both = step_v[rows, :].astype(F32) + recv_v[rows, :].astype(F32)
        out_ref[rows, :] = (both * 0.5).astype(BF16)
    for i in range(len(late)):
        step_copy(i).wait_send()
    for copy in (early_w, early_s, slope_copy, slope_pass, fact_copy):
        copy.wait_send()


def one_round(n_nodes, n_tp, level, states, weights, gain, upstream, cosine, sine):
    tokens, local = states.shape
    columns = weights.shape[1]
    width = columns // 3
    pieces, parts = 16, len(token_blocks(tokens))
    early = local // pieces * (5, 2, 2, 1)[min(level, 3)]
    vmem = pl.BlockSpec(memory_space=pltpu.VMEM)
    anywhere = pl.BlockSpec(memory_space=pl.ANY)
    dma = pltpu.SemaphoreType.DMA
    flops = 4 * tokens * local * columns + 12 * tokens * tokens * columns // 3
    return pl.pallas_call(
        functools.partial(kernel, n_nodes, n_tp, 1 << level, early),
        out_shape=jax.ShapeDtypeStruct(weights.shape, BF16),
        in_specs=[anywhere] * 6,
        out_specs=vmem,
        scratch_shapes=[
            pltpu.VMEM((tokens, local), BF16),
            pltpu.VMEM((local, columns), BF16),
            pltpu.VMEM(gain.shape, F32),
            pltpu.VMEM((tokens, width), BF16),
            pltpu.VMEM((tokens, width), F32),
            pltpu.VMEM((tokens, width), F32),
            pltpu.VMEM((tokens, local), BF16),
            pltpu.VMEM((local, tokens), BF16),
            pltpu.VMEM((tokens, columns), F32),
            pltpu.VMEM((tokens, columns), BF16),
            pltpu.VMEM((tokens, columns), BF16),
            pltpu.VMEM((parts, 8, 128), F32),
            pltpu.VMEM((parts, 8, 128), F32),
            pltpu.VMEM((8, 128), F32),
            pltpu.VMEM((8, 128), F32),
            pltpu.VMEM((tokens, width), BF16),
            pltpu.VMEM((tokens, width), BF16),
            pltpu.VMEM((tokens, width), F32),
            pltpu.VMEM((tokens, width), F32),
            pltpu.VMEM((tokens, columns), BF16),
            pltpu.VMEM((local, columns), F32),
            pltpu.VMEM((local, columns), BF16),
            pltpu.VMEM((local, columns), BF16),
            pltpu.VMEM((tokens, early), BF16),
            pltpu.VMEM((early, columns), BF16),
            pltpu.VMEM((early, tokens), BF16),
            pltpu.VMEM((tokens, columns), BF16),
            pltpu.VMEM((8, 128), F32),
            pltpu.VMEM((8, 128), F32),
            dma((parts + 5,)),
            dma((parts,)),
            dma((parts,)),
            dma((parts,)),
            dma((parts,)),
            dma((2,)),
            dma((pieces,)),
            dma((pieces,)),
            dma((2,)),
            dma((2,)),
            dma((2,)),
            dma((2,)),
            dma((2,)),
        ],
        compiler_params=pltpu.CompilerParams(
            collective_id=level, has_side_effects=True, vmem_limit_bytes=60 * 2**20
        ),
        cost_estimate=pl.CostEstimate(
            flops=flops, bytes_accessed=6 * local * columns + 2 * tokens * local, transcendentals=0
        ),
        name="gossip",
    )(states, weights, gain, upstream, cosine, sine)


def solution(mesh):
    n_nodes, n_tp = mesh.shape["node"], mesh.shape["tp"]
    levels = n_nodes.bit_length() - 1

    def per_device(states, weights, norm_gain, cotangent, round_index):
        cosine, sine = rope_tables(cotangent.shape[1], cotangent.shape[2])
        exponent = round_index[0] % levels
        branches = [functools.partial(one_round, n_nodes, n_tp, level) for level in range(levels)]
        out = lax.switch(
            exponent, branches,
            states[0], weights[0], norm_gain[None, :], cotangent[0], cosine, sine,
        )
        return out[None]

    return jax.shard_map(
        per_device,
        mesh=mesh,
        in_specs=(
            P("node", None, "tp"),
            P("node", "tp", None),
            P("tp"),
            P("node", None, None),
            P(),
        ),
        out_specs=P("node", "tp", None),
        check_vma=False,
    )
```
